32 devices in a mesh: ka: 8 (over z, y), ga: 4 (over x, core).
Axes of the slice: x: 2, y: 2, z: 4, core: 2. Of those that a mesh axis runs over, the one named last changes fastest.
Arguments:
- x_dens: bfloat16 [32, 64, 1500], P('ka', None, 'ga'), may hold values from -6 to 6
- y_dens: bfloat16 [32, 64, 1500], P('ka', None, 'ga'), may hold values from -0.15625 to 0.15625
- p_dens: bfloat16 [32, 64, 1500], P('ka', None, 'ga'), may hold values from -1 to 1
- coulomb: float32 [1500], P('ga'), may hold values from 0.1 to 2
- screened: bfloat16 [16, 1500, 1500], P('ka', 'ga'), may hold values from -0.15625 to 0.15625
- pairs: int32 [128, 3], P('ka'), may hold values from 0 to 31, as said below
- q_slot: int32 [16], replicated, may hold values from 0 to 15, as said below
Outputs:
- blocks: float32 [128, 4096], P('ka')
- mirrored: float32 [32, 4096], P('ka')
The draws below stay inside these ranges and needn't reach their ends.
Inputs may be any that keep to these rules, and one draw needn't show every extreme that they name: `pairs`: column 0 of the rows held by index d of ka lies in d * 4 to (d + 1) * 4 - 1; column 1 is any k-point; column 2 is a momentum transfer below 16. Among one index's 16 rows at most 2 have a second k-point held by one same index, and this is reached; at most 2 have q_slot[q] // 2 equal to one same value, and this is reached. `q_slot`: A permutation of the slots; slot s of screened is held by index s // 2 of ka.
All inputs are finite; a program needn't handle non-finite values.
Results may differ from the reference program's by a relative error of at most 0.0014.
Values may be sent and summed in bfloat16 or wider, within the bound.
A program may use at most 192 MiB of HBM per device.

```python
import math
import jax
import jax.numpy as jnp
from jax import lax

NT = 64
NG = 1500
K_DEV = 4
PAIR_DEV = 16
QS = 2
CAPQ = 2
CAPK = 2
K_ALL = 32
NQ = 16
PAIRS = 128
N_KA = 8


def shared_slots(key):
    return jax.random.permutation(jax.random.fold_in(key, 7), NQ).astype(jnp.int32)


def draw_q_slot(key, part):
    return shared_slots(key)


def draw_pairs(key, part):
    slot_of = shared_slots(key)
    inverse = jnp.zeros((NQ,), jnp.int32).at[slot_of].set(jnp.arange(NQ, dtype=jnp.int32))
    popular = jax.random.permutation(jax.random.fold_in(key, 9), N_KA) < max(1, N_KA // 8)

    def one_block(index):
        block_key = jax.random.fold_in(key, 100 + index)
        keys = jax.random.split(block_key, 7)
        firsts = index * K_DEV + jax.random.randint(keys[0], (PAIR_DEV,), 0, K_DEV)
        k_owners = jax.random.permutation(keys[1], N_KA)[jnp.arange(PAIR_DEV) // CAPK]
        k_owners = k_owners[jax.random.permutation(keys[2], PAIR_DEV)]
        seconds = k_owners * K_DEV + jax.random.randint(keys[3], (PAIR_DEV,), 0, K_DEV)
        scores = jax.random.randint(keys[4], (N_KA,), 0, 1000) + 800 * popular.astype(jnp.int32)
        scores = scores * N_KA + jnp.arange(N_KA, dtype=jnp.int32)
        ranking = jnp.argsort(-scores, stable=True).astype(jnp.int32)
        q_owners = ranking[jnp.arange(PAIR_DEV) // CAPQ]
        q_owners = q_owners[jax.random.permutation(keys[5], PAIR_DEV)]
        slots = q_owners * QS + jax.random.randint(keys[6], (PAIR_DEV,), 0, QS)
        transfers = inverse[slots]
        return jnp.stack([firsts, seconds, transfers], axis=1).astype(jnp.int32)
    return jax.vmap(one_block)(jnp.arange(N_KA, dtype=jnp.int32)).reshape(PAIRS, 3)


def block_levels(stream_key, dims, cuts, smallest, largest):
    level = 1.0
    for dim, shards_of in cuts:
        draws = jax.random.uniform(jax.random.fold_in(jax.random.fold_in(stream_key, 6), dim), (shards_of,), jnp.float32, smallest / len(cuts), largest / len(cuts))
        level = level * jnp.repeat(jnp.exp(draws), dims[dim] // shards_of).reshape((-1,) + (1,) * (len(dims) - 1 - dim))
    return level


def gaussian(own_key, shape, scale, reach, pieces=(), held_as=jnp.bfloat16):
    entries = jax.random.normal(own_key, shape, jnp.float32) * scale
    if len(pieces) > 0:
        entries = block_levels(own_key, shape, pieces, -0.22, 0.18) * entries
    return jnp.clip(entries, min=-reach, max=reach).astype(held_as)


def setup_inputs(seed: int = 0) -> dict:
    arg_keys = jax.random.split(jax.random.key(seed), 8)
    x_dens = gaussian(arg_keys[0], (K_ALL, NT, NG), 1.0, 6.0, ((0, 8), (2, 4)))
    y_dens = gaussian(arg_keys[1], (K_ALL, NT, NG), NG ** -0.5, 0.15625, ((0, 8), (2, 4)))
    p_dens = gaussian(arg_keys[2], (K_ALL, NT, NG), 0.16, 1.0, ((0, 8), (2, 4)))
    coulomb = jnp.clip(jnp.exp(math.log(2.0) - 2.9957323 * jax.random.uniform(arg_keys[3], (NG,), jnp.float32) ** block_levels(arg_keys[3], (NG,), ((0, 4),), -0.2, 0.2)), 0.1, 2.0)
    screened = gaussian(arg_keys[4], (NQ, NG, NG), NG ** -0.5, 0.15625, ((0, 8), (1, 4)))
    pairs = draw_pairs(jax.random.fold_in(arg_keys[7], 71), 0)
    q_slot = draw_q_slot(jax.random.fold_in(arg_keys[7], 71), 0)
    return {"x_dens": x_dens, "y_dens": y_dens, "p_dens": p_dens, "coulomb": coulomb, "screened": screened, "pairs": pairs, "q_slot": q_slot}


def reference(x_dens, y_dens, p_dens, coulomb, screened, pairs, q_slot):
    def one_pair(entry):
        k_index = entry[0]
        partner = entry[1]
        q_index = entry[2]
        w_matrix = screened[q_slot[q_index]]
        half_rows = jnp.dot(x_dens[k_index], w_matrix, preferred_element_type=jnp.float32).astype(jnp.bfloat16)
        direct = jnp.dot(half_rows, y_dens[partner].T, preferred_element_type=jnp.float32)
        weighted = p_dens[k_index].astype(jnp.float32) * coulomb[None, :]
        exchange_term = jnp.dot(weighted, p_dens[partner].astype(jnp.float32).T, precision=lax.Precision.HIGHEST)
        return 2.0 * exchange_term - direct

    kernel_blocks = lax.map(one_pair, pairs)
    flipped = jnp.transpose(kernel_blocks, (0, 2, 1)).reshape(PAIRS, NT * NT)
    mirrored = jax.ops.segment_sum(flipped, pairs[:, 1].astype(jnp.int32), num_segments=K_DEV * N_KA)
    return kernel_blocks.reshape(PAIRS, NT * NT), mirrored
```

```python
import functools
import jax
import jax.numpy as jnp
from jax import lax
from jax.experimental import pallas as pl
from jax.experimental.pallas import tpu as pltpu
from jax.sharding import PartitionSpec as P

CAPQ = 2
F32 = jnp.float32
BF16 = jnp.bfloat16
VM = pl.BlockSpec(memory_space=pltpu.VMEM)
SM = pl.BlockSpec(memory_space=pltpu.SMEM)
LIMIT = 66000000


class Gather:
    def __init__(self, n, src, out, send, recv):
        self.n, self.nz = n, n // 2
        self.me = lax.axis_index("ka")
        self.z, self.y = self.me // 2, self.me % 2
        self.src, self.out, self.send, self.recv = src, out, send, recv
        self.size = src.shape[0]
        self.half = self.size // 2

    def copy(self, zz, yy, half, way, own=False):
        block = self.out.at[pl.ds((zz * 2 + yy) * self.size + half * self.half, self.half)]
        source = self.src.at[pl.ds(half * self.half, self.half)] if own else block
        index = (zz * 2 + yy) * 2 + half
        if way == 2:
            target = self.z * 2 + 1 - self.y
        else:
            step = 1 if way == 0 else -1
            target = (self.z + step) * 2 + self.y
        return pltpu.make_async_remote_copy(
            src_ref=source,
            dst_ref=block,
            send_sem=self.send.at[way * 2 * self.n + index],
            recv_sem=self.recv.at[index],
            device_id={"ka": target},
            device_id_type=pl.DeviceIdType.MESH,
        )

    def chain(self, zz, yy, half, act, ways=(0, 1), own=False):
        for way in ways:
            free = self.z < self.nz - 1 if way == 0 else self.z > 0

            @pl.when(free)
            def _(way=way):
                act(self.copy(zz, yy, half, way, own))

    def first(self):
        start = lambda c: c.start()
        self.copy(self.z, self.y, 1, 2, True).start()
        self.chain(self.z, self.y, 0, start, own=True)
        self.chain(self.z, self.y, 1, start, own=True)
        self.copy(self.z, self.y, 0, 2, True).start()
        self.out[pl.ds(self.me * self.size, self.size)] = self.src[...]

    def second(self):
        start = lambda c: c.start()
        self.copy(self.z, 1 - self.y, 1, 2).wait_recv()
        self.chain(self.z, 1 - self.y, 1, start)

    def hop(self, h):
        start = lambda c: c.start()
        for way in (0, 1):
            zz = self.z - h if way == 0 else self.z + h
            there = zz >= 0 if way == 0 else zz < self.nz

            @pl.when(there)
            def _(zz=zz, way=way):
                for yy, half in ((self.y, 0), (self.y, 1), (1 - self.y, 1)):
                    self.copy(zz, yy, half, 2).wait_recv()
                    self.chain(zz, yy, half, start, (way,))
                    if half == 0:
                        self.copy(zz, yy, 0, 2).start()

    def finish(self):
        done = lambda c: c.wait_send()
        self.copy(self.z, self.y, 1, 2, True).wait_send()
        for half in (0, 1):
            self.chain(self.z, self.y, half, done, own=True)
        self.copy(self.z, self.y, 0, 2, True).wait_send()
        self.chain(self.z, 1 - self.y, 1, done)
        self.copy(self.z, 1 - self.y, 0, 2).wait_recv()

        def tail(h, carry):
            for way in (0, 1):
                zz = self.z - h if way == 0 else self.z + h
                there = zz >= 0 if way == 0 else zz < self.nz

                @pl.when(there)
                def _(zz=zz, way=way):
                    for yy, half in ((self.y, 0), (self.y, 1), (1 - self.y, 1)):
                        self.chain(zz, yy, half, done, (way,))
                    self.copy(zz, self.y, 0, 2).wait_send()
                    self.copy(zz, 1 - self.y, 0, 2).wait_recv()

            return carry

        lax.fori_loop(1, self.nz, tail, 0)


def run_gathers(gathers, between=None):
    for g in gathers:
        g.first()
    for g in gathers:
        g.second()
    if between is not None:
        between()

    def body(h, carry):
        for g in gathers:
            g.hop(h)
        return carry

    lax.fori_loop(1, gathers[0].nz, body, 0)
    for g in gathers:
        g.finish()


def greet(n, ka_too, ga_too):
    barrier = pltpu.get_barrier_semaphore()
    me = lax.axis_index("ka")
    z, y = me // 2, me % 2
    nz = n // 2
    targets = []
    if ka_too:
        targets += [{"ka": lax.rem(z + 1, nz) * 2 + y}, {"ka": lax.rem(z + nz - 1, nz) * 2 + y}]
        targets += [{"ka": z * 2 + 1 - y}]
    if ga_too:
        g = lax.axis_index("ga")
        n_ga = lax.axis_size("ga")
        targets += [{"ga": lax.rem(g + i, n_ga)} for i in range(1, n_ga)]
    for t in targets:
        pl.semaphore_signal(barrier, inc=1, device_id=t, device_id_type=pl.DeviceIdType.MESH)
    pl.semaphore_wait(barrier, len(targets))


def gather_sems(n):
    return [pltpu.SemaphoreType.DMA((6 * n,)), pltpu.SemaphoreType.DMA((2 * n,))]


def params(collective_id):
    return pltpu.CompilerParams(
        collective_id=collective_id, has_side_effects=True, vmem_limit_bytes=LIMIT
    )


def first_kernel(n, x_ref, l_ref, xo_ref, lo_ref, xs, xr, ls, lr):
    greet(n, True, False)
    run_gathers([Gather(n, l_ref, lo_ref, ls, lr), Gather(n, x_ref, xo_ref, xs, xr)])


def half_kernel(n, rows, q_slots, list_ref, qs_ref, x_ref, w_ref, o_ref, k_ref, k2_ref, at_ref, w_at, count):
    me = lax.axis_index("ka")
    slots = n * CAPQ

    def clear(s, c):
        k_ref[s] = 0
        k2_ref[s] = 0
        w_at[s] = 0
        return c

    lax.fori_loop(0, slots, clear, 0)

    def source(a, c):
        def zero(o, c):
            count[o] = 0
            return c

        lax.fori_loop(0, n, zero, 0)

        def pair(j, c):
            r = a * rows + j
            slot = qs_ref[list_ref[r * 3 + 2]]
            owner = slot // q_slots
            rank = count[owner]
            count[owner] = rank + 1
            at_ref[r] = owner * CAPQ + rank

            @pl.when(owner == me)
            def _():
                s = a * CAPQ + rank
                k_ref[s] = list_ref[r * 3]
                k2_ref[s] = list_ref[r * 3 + 1]
                w_at[s] = slot % q_slots

            return c

        return lax.fori_loop(0, rows, pair, c)

    lax.fori_loop(0, n, source, 0)
    n_ga, g = o_ref.shape[0], o_ref.shape[3]

    def multiply(s, c):
        v = jnp.dot(x_ref[k_ref[s]], w_ref[w_at[s]], preferred_element_type=F32)
        for i in range(n_ga):
            o_ref[i, s] = v[:, i * g : (i + 1) * g].astype(o_ref.dtype)
        return c

    lax.fori_loop(0, slots, multiply, 0)


def reduce_two(part, out, recv1, tsend, recv2, s1, r1, s2, r2, pieces):
    g = lax.axis_index("ga")
    x, c = g // 2, g % 2
    per = part.shape[1] // pieces
    there, here = 1 - x, x

    def one(t, xx, i):
        rows = pl.ds(i * per, per)
        return pltpu.make_async_remote_copy(
            src_ref=part.at[xx * 2 + 1 - c, rows],
            dst_ref=recv1.at[xx, rows],
            send_sem=s1.at[t * pieces + i],
            recv_sem=r1.at[t * pieces + i],
            device_id={"ga": x * 2 + 1 - c},
            device_id_type=pl.DeviceIdType.MESH,
        )

    def two(i):
        rows = pl.ds(i * per, per)
        return pltpu.make_async_remote_copy(
            src_ref=tsend.at[rows],
            dst_ref=recv2.at[rows],
            send_sem=s2.at[i],
            recv_sem=r2.at[i],
            device_id={"ga": there * 2 + c},
            device_id_type=pl.DeviceIdType.MESH,
        )

    def begin():
        for i in range(pieces):
            one(0, there, i).start()
        for i in range(pieces):
            one(1, here, i).start()

    def middle():
        for i in range(pieces):
            rows = pl.ds(i * per, per)
            one(0, there, i).wait_recv()
            v = part[there * 2 + c, rows].astype(F32) + recv1[there, rows].astype(F32)
            tsend[rows] = v.astype(tsend.dtype)
            two(i).start()

    def end():
        for i in range(pieces):
            rows = pl.ds(i * per, per)
            one(1, here, i).wait_recv()
            two(i).wait_recv()
            v = part[here * 2 + c, rows].astype(F32) + recv1[here, rows].astype(F32)
            out[rows] = (v + recv2[rows].astype(F32)).astype(out.dtype)
        for i in range(pieces):
            one(0, there, i).wait_send()
            one(1, here, i).wait_send()
            two(i).wait_send()

    return begin, middle, end


def second_kernel(n, pieces, part, y_ref, p_ref, half_ref, yo_ref, po_ref, recv1, tsend, recv2,
                  s1, r1, s2, r2, ys, yr, ps, pr):
    greet(n, True, True)
    begin, middle, end = reduce_two(part, half_ref, recv1, tsend, recv2, s1, r1, s2, r2, pieces)
    begin()
    run_gathers([Gather(n, y_ref, yo_ref, ys, yr), Gather(n, p_ref, po_ref, ps, pr)], middle)
    end()


def block_kernel(n, k_ref, k2_ref, half_ref, y_ref, p_ref, v_ref, o_ref):
    n_ga, quarter = o_ref.shape[0], o_ref.shape[2]
    dims = (((1,), (1,)), ((), ()))

    def source(a, carry):
        both = []
        for c in range(CAPQ):
            s = a * CAPQ + c
            k, k2 = k_ref[s], k2_ref[s]
            direct = lax.dot_general(half_ref[s], y_ref[k2], dims, preferred_element_type=F32)
            weighted = p_ref[k].astype(F32) * v_ref[...]
            high = weighted.astype(BF16)
            low = (weighted - high.astype(F32)).astype(BF16)
            other = p_ref[k2]
            term = lax.dot_general(high, other, dims, preferred_element_type=F32)
            term += lax.dot_general(low, other, dims, preferred_element_type=F32)
            both.append(2.0 * term - direct)
        v = jnp.concatenate(both, axis=1)
        for i in range(n_ga):
            o_ref[i, a] = v[i * quarter : (i + 1) * quarter]
        return carry

    lax.fori_loop(0, n, source, 0)


def third_kernel(n, part, all_ref, own, recv1, tsend, recv2, s1, r1, s2, r2, gs, gr):
    greet(n, True, True)
    begin, middle, end = reduce_two(part, own, recv1, tsend, recv2, s1, r1, s2, r2, 1)
    begin()
    middle()
    end()
    run_gathers([Gather(n, own, all_ref, gs, gr)])


def select_kernel(n, rows, per_dev, list_ref, at_ref, all_ref, o_ref, acc):
    me = lax.axis_index("ka")
    nt = all_ref.shape[2] // CAPQ

    def tile(a, j):
        at = at_ref[a * rows + j]
        both = all_ref[(at // CAPQ) * n + a]
        return jnp.where(at % CAPQ == 0, both[:, :nt], both[:, nt:])

    for j in range(rows // 2):
        o_ref[j] = jnp.concatenate([tile(me, j), tile(me, j + rows // 2)], axis=1)
    acc[...] = jnp.zeros_like(acc)

    def pair(r, c):
        second = list_ref[r * 3 + 1] - me * per_dev

        @pl.when(jnp.logical_and(second >= 0, second < per_dev))
        def _():
            a = r // rows
            acc[second] = acc[second] + tile(a, r - a * rows)

        return c

    lax.fori_loop(0, n * rows, pair, 0)
    for k in range(per_dev // 2):
        o_ref[rows // 2 + k] = jnp.concatenate([acc[k], acc[k + per_dev // 2]], axis=1)


def fourth_kernel(n, src, out, send, recv):
    greet(n, False, True)
    g = lax.axis_index("ga")
    n_ga = out.shape[0]
    copies = [
        pltpu.make_async_remote_copy(
            src_ref=src,
            dst_ref=out.at[g],
            send_sem=send.at[i],
            recv_sem=recv.at[i],
            device_id={"ga": lax.rem(g + i, n_ga)},
            device_id_type=pl.DeviceIdType.MESH,
        )
        for i in range(1, n_ga)
    ]
    for c in copies:
        c.start()
    out[g] = src[...]
    for c in copies:
        c.wait()


def per_device(x_dens, y_dens, p_dens, coulomb, screened, pairs, q_slot):
    n = lax.axis_size("ka")
    n_ga = lax.axis_size("ga")
    per_dev, nt, g = x_dens.shape
    q_slots = screened.shape[0]
    rows = pairs.shape[0]
    slots = n * CAPQ
    shape = jax.ShapeDtypeStruct
    listed = jnp.pad(pairs, ((0, 0), (0, 128 - pairs.shape[1]))).reshape(2, rows // 2, 128)
    x_all, listed = pl.pallas_call(
        functools.partial(first_kernel, n),
        out_shape=[shape((n * per_dev, nt, g), BF16), shape((n * 2, rows // 2, 128), jnp.int32)],
        in_specs=[VM, VM],
        out_specs=[VM, VM],
        scratch_shapes=gather_sems(n) + gather_sems(n),
        compiler_params=params(0),
        name="gather_x",
    )(x_dens, listed)
    listed = listed.reshape(n * rows, 128)[:, :3].reshape(n * rows * 3)
    wide = F32 if slots * nt <= 2048 else BF16
    ints = lambda m: shape((m,), jnp.int32)
    part, k_at, k2_at, at = pl.pallas_call(
        functools.partial(half_kernel, n, rows, q_slots),
        out_shape=[shape((n_ga, slots, nt, g), wide), ints(slots), ints(slots), ints(n * rows)],
        in_specs=[SM, SM, VM, VM],
        out_specs=[VM, SM, SM, SM],
        scratch_shapes=[pltpu.SMEM((slots,), jnp.int32), pltpu.SMEM((n,), jnp.int32)],
        compiler_params=pltpu.CompilerParams(vmem_limit_bytes=LIMIT),
        name="half",
    )(listed, q_slot, x_all, screened)
    pieces = 4
    half, y_all, p_all = pl.pallas_call(
        functools.partial(second_kernel, n, pieces),
        out_shape=[shape((slots, nt, g), BF16)] + [shape((n * per_dev, nt, g), BF16)] * 2,
        in_specs=[VM, VM, VM],
        out_specs=[VM, VM, VM],
        scratch_shapes=[
            pltpu.VMEM((2, slots, nt, g), wide),
            pltpu.VMEM((slots, nt, g), BF16),
            pltpu.VMEM((slots, nt, g), BF16),
            pltpu.SemaphoreType.DMA((2 * pieces,)),
            pltpu.SemaphoreType.DMA((2 * pieces,)),
            pltpu.SemaphoreType.DMA((pieces,)),
            pltpu.SemaphoreType.DMA((pieces,)),
        ]
        + gather_sems(n)
        + gather_sems(n),
        compiler_params=params(1),
        name="reduce_gather",
    )(part, y_dens, p_dens)
    quarter = nt // n_ga
    block = pl.pallas_call(
        functools.partial(block_kernel, n),
        out_shape=shape((n_ga, n, quarter, CAPQ * nt), F32),
        in_specs=[SM, SM, VM, VM, VM, VM],
        out_specs=VM,
        compiler_params=pltpu.CompilerParams(vmem_limit_bytes=LIMIT),
        name="block",
    )(k_at, k2_at, half, y_all, p_all, coulomb.reshape(1, g))
    line = (n, quarter, CAPQ * nt)
    everything = pl.pallas_call(
        functools.partial(third_kernel, n),
        out_shape=shape((n * n, quarter, CAPQ * nt), F32),
        in_specs=[VM],
        out_specs=VM,
        scratch_shapes=[
            pltpu.VMEM(line, F32),
            pltpu.VMEM((2,) + line, F32),
            pltpu.VMEM(line, F32),
            pltpu.VMEM(line, F32),
        ]
        + [pltpu.SemaphoreType.DMA((2,))] * 4
        + gather_sems(n),
        compiler_params=params(2),
        name="reduce_blocks",
    )(block)
    lines = rows // 2 + per_dev // 2
    mine = pl.pallas_call(
        functools.partial(select_kernel, n, rows, per_dev),
        out_shape=shape((lines, quarter, 2 * nt), F32),
        in_specs=[SM, SM, VM],
        out_specs=VM,
        scratch_shapes=[pltpu.VMEM((per_dev, quarter, nt), F32)],
        compiler_params=pltpu.CompilerParams(vmem_limit_bytes=LIMIT),
        name="select",
    )(listed, at, everything)
    full = pl.pallas_call(
        functools.partial(fourth_kernel, n),
        out_shape=shape((n_ga, lines, quarter, 2 * nt), F32),
        in_specs=[VM],
        out_specs=VM,
        scratch_shapes=[pltpu.SemaphoreType.DMA((n_ga,))] * 2,
        compiler_params=params(3),
        name="gather_out",
    )(mine)
    split = lambda v: jnp.concatenate([v[..., :nt], v[..., nt:]], axis=1)
    blocks = split(full[:, : rows // 2]).transpose(1, 0, 2, 3).reshape(rows, nt * nt)
    mirrored = split(full[:, rows // 2 :]).transpose(1, 3, 0, 2).reshape(per_dev, nt * nt)
    return (blocks, mirrored)


def solution(mesh):
    in_specs = (
        P("ka", None, "ga"),
        P("ka", None, "ga"),
        P("ka", None, "ga"),
        P("ga"),
        P("ka", "ga", None),
        P("ka", None),
        P(),
    )
    out_specs = (P("ka", None), P("ka", None))
    return jax.shard_map(
        per_device, mesh=mesh, in_specs=in_specs, out_specs=out_specs, check_vma=False
    )
```

```python
import functools
import jax
import jax.numpy as jnp
from jax import lax
from jax.experimental import pallas as pl
from jax.experimental.pallas import tpu as pltpu
from jax.sharding import PartitionSpec as P

CAPQ = 2
F32 = jnp.float32
BF16 = jnp.bfloat16
VM = pl.BlockSpec(memory_space=pltpu.VMEM)
SM = pl.BlockSpec(memory_space=pltpu.SMEM)
LIMIT = 66000000


class Gather:
    def __init__(self, n, src, out, send, recv):
        self.n, self.nz = n, n // 2
        self.me = lax.axis_index("ka")
        self.z, self.y = self.me // 2, self.me % 2
        self.src, self.out, self.send, self.recv = src, out, send, recv
        self.size = src.shape[0]
        self.cut = self.size - max(1, self.size // 6)

    def copy(self, zz, yy, half, way, own=False):
        first, length = (self.cut, self.size - self.cut) if half else (0, self.cut)
        block = self.out.at[pl.ds((zz * 2 + yy) * self.size + first, length)]
        source = self.src.at[pl.ds(first, length)] if own else block
        index = (zz * 2 + yy) * 2 + half
        if way == 2:
            target = self.z * 2 + 1 - self.y
        else:
            step = 1 if way == 0 else -1
            target = (self.z + step) * 2 + self.y
        return pltpu.make_async_remote_copy(
            src_ref=source,
            dst_ref=block,
            send_sem=self.send.at[way * 2 * self.n + index],
            recv_sem=self.recv.at[index],
            device_id={"ka": target},
            device_id_type=pl.DeviceIdType.MESH,
        )

    def chain(self, zz, yy, half, act, ways=(0, 1), own=False):
        for way in ways:
            free = self.z < self.nz - 1 if way == 0 else self.z > 0

            @pl.when(free)
            def _(way=way):
                act(self.copy(zz, yy, half, way, own))

    def first(self):
        start = lambda c: c.start()
        self.copy(self.z, self.y, 1, 2, True).start()
        self.chain(self.z, self.y, 0, start, own=True)
        self.chain(self.z, self.y, 1, start, own=True)
        self.copy(self.z, self.y, 0, 2, True).start()
        self.out[pl.ds(self.me * self.size, self.size)] = self.src[...]

    def second(self):
        start = lambda c: c.start()
        self.copy(self.z, 1 - self.y, 1, 2).wait_recv()
        self.chain(self.z, 1 - self.y, 1, start)

    def hop(self, h):
        start = lambda c: c.start()
        for way in (0, 1):
            zz = self.z - h if way == 0 else self.z + h
            there = zz >= 0 if way == 0 else zz < self.nz

            @pl.when(there)
            def _(zz=zz, way=way):
                for yy, half in ((self.y, 0), (self.y, 1), (1 - self.y, 1)):
                    self.copy(zz, yy, half, 2).wait_recv()
                    self.chain(zz, yy, half, start, (way,))
                    if half == 0:
                        self.copy(zz, yy, 0, 2).start()

    def finish(self):
        done = lambda c: c.wait_send()
        self.copy(self.z, self.y, 1, 2, True).wait_send()
        for half in (0, 1):
            self.chain(self.z, self.y, half, done, own=True)
        self.copy(self.z, self.y, 0, 2, True).wait_send()
        self.chain(self.z, 1 - self.y, 1, done)
        self.copy(self.z, 1 - self.y, 0, 2).wait_recv()

        def tail(h, carry):
            for way in (0, 1):
                zz = self.z - h if way == 0 else self.z + h
                there = zz >= 0 if way == 0 else zz < self.nz

                @pl.when(there)
                def _(zz=zz, way=way):
                    for yy, half in ((self.y, 0), (self.y, 1), (1 - self.y, 1)):
                        self.chain(zz, yy, half, done, (way,))
                    self.copy(zz, self.y, 0, 2).wait_send()
                    self.copy(zz, 1 - self.y, 0, 2).wait_recv()

            return carry

        lax.fori_loop(1, self.nz, tail, 0)


def run_gathers(gathers, between=None):
    for g in gathers:
        g.first()
    for g in gathers:
        g.second()
    if between is not None:
        between()

    def body(h, carry):
        for g in gathers:
            g.hop(h)
        return carry

    lax.fori_loop(1, gathers[0].nz, body, 0)
    for g in gathers:
        g.finish()


def greet(n, ka_too, ga_too, all_ka=False):
    barrier = pltpu.get_barrier_semaphore()
    me = lax.axis_index("ka")
    z, y = me // 2, me % 2
    nz = n // 2
    targets = []
    if ka_too:
        targets += [{"ka": lax.rem(z + 1, nz) * 2 + y}, {"ka": lax.rem(z + nz - 1, nz) * 2 + y}]
        targets += [{"ka": z * 2 + 1 - y}]
    if all_ka:
        targets += [{"ka": lax.rem(me + i, n)} for i in range(1, n)]
    if ga_too:
        g = lax.axis_index("ga")
        n_ga = lax.axis_size("ga")
        targets += [{"ga": lax.rem(g + i, n_ga)} for i in range(1, n_ga)]
    for t in targets:
        pl.semaphore_signal(barrier, inc=1, device_id=t, device_id_type=pl.DeviceIdType.MESH)
    pl.semaphore_wait(barrier, len(targets))


def gather_sems(n):
    return [pltpu.SemaphoreType.DMA((6 * n,)), pltpu.SemaphoreType.DMA((2 * n,))]


def params(collective_id):
    return pltpu.CompilerParams(
        collective_id=collective_id, has_side_effects=True, vmem_limit_bytes=LIMIT
    )


def first_kernel(n, x_ref, l_ref, xo_ref, lo_ref, xs, xr, ls, lr):
    greet(n, True, False)
    run_gathers([Gather(n, l_ref, lo_ref, ls, lr), Gather(n, x_ref, xo_ref, xs, xr)])


def half_kernel(n, rows, q_slots, list_ref, qs_ref, x_ref, w_ref, o_ref, k_ref, k2_ref, at_ref, w_at, count):
    me = lax.axis_index("ka")
    slots = n * CAPQ

    def clear(s, c):
        k_ref[s] = 0
        k2_ref[s] = -1
        w_at[s] = 0
        return c

    lax.fori_loop(0, slots, clear, 0)

    def source(a, c):
        def zero(o, c):
            count[o] = 0
            return c

        lax.fori_loop(0, n, zero, 0)

        def pair(j, c):
            r = a * rows + j
            slot = qs_ref[list_ref[r * 3 + 2]]
            owner = slot // q_slots
            rank = count[owner]
            count[owner] = rank + 1
            at_ref[r] = owner * CAPQ + rank

            @pl.when(owner == me)
            def _():
                s = a * CAPQ + rank
                k_ref[s] = list_ref[r * 3]
                k2_ref[s] = list_ref[r * 3 + 1]
                w_at[s] = slot % q_slots

            return c

        return lax.fori_loop(0, rows, pair, c)

    lax.fori_loop(0, n, source, 0)
    n_ga, g = o_ref.shape[0], o_ref.shape[3]

    def multiply(s, c):
        v = jnp.dot(x_ref[k_ref[s]], w_ref[w_at[s]], preferred_element_type=F32)
        for i in range(n_ga):
            o_ref[i, s] = v[:, i * g : (i + 1) * g].astype(o_ref.dtype)
        return c

    lax.fori_loop(0, slots, multiply, 0)


def reduce_two(part, out, recv1, tsend, recv2, s1, r1, s2, r2, pieces):
    g = lax.axis_index("ga")
    x, c = g // 2, g % 2
    per = part.shape[1] // pieces
    there, here = 1 - x, x

    def one(t, xx, i):
        rows = pl.ds(i * per, per)
        return pltpu.make_async_remote_copy(
            src_ref=part.at[xx * 2 + 1 - c, rows],
            dst_ref=recv1.at[xx, rows],
            send_sem=s1.at[t * pieces + i],
            recv_sem=r1.at[t * pieces + i],
            device_id={"ga": x * 2 + 1 - c},
            device_id_type=pl.DeviceIdType.MESH,
        )

    def two(i):
        rows = pl.ds(i * per, per)
        return pltpu.make_async_remote_copy(
            src_ref=tsend.at[rows],
            dst_ref=recv2.at[rows],
            send_sem=s2.at[i],
            recv_sem=r2.at[i],
            device_id={"ga": there * 2 + c},
            device_id_type=pl.DeviceIdType.MESH,
        )

    def begin():
        for i in range(pieces):
            one(0, there, i).start()
        for i in range(pieces):
            one(1, here, i).start()

    def middle():
        for i in range(pieces):
            rows = pl.ds(i * per, per)
            one(0, there, i).wait_recv()
            v = part[there * 2 + c, rows].astype(F32) + recv1[there, rows].astype(F32)
            tsend[rows] = v.astype(tsend.dtype)
            two(i).start()

    def end():
        for i in range(pieces):
            rows = pl.ds(i * per, per)
            one(1, here, i).wait_recv()
            two(i).wait_recv()
            v = part[here * 2 + c, rows].astype(F32) + recv1[here, rows].astype(F32)
            out[rows] = (v + recv2[rows].astype(F32)).astype(out.dtype)
        for i in range(pieces):
            one(0, there, i).wait_send()
            one(1, here, i).wait_send()
            two(i).wait_send()

    return begin, middle, end


def second_kernel(n, pieces, part, y_ref, p_ref, half_ref, yo_ref, po_ref, recv1, tsend, recv2,
                  s1, r1, s2, r2, ys, yr, ps, pr):
    greet(n, True, True)
    begin, middle, end = reduce_two(part, half_ref, recv1, tsend, recv2, s1, r1, s2, r2, pieces)
    begin()
    run_gathers([Gather(n, y_ref, yo_ref, ys, yr), Gather(n, p_ref, po_ref, ps, pr)], middle)
    end()


def block_kernel(n, k_ref, k2_ref, half_ref, y_ref, p_ref, v_ref, o_ref):
    n_ga, quarter = o_ref.shape[0], o_ref.shape[2]
    dims = (((1,), (1,)), ((), ()))

    def source(a, carry):
        both = []
        for c in range(CAPQ):
            s = a * CAPQ + c
            k, k2 = k_ref[s], jnp.maximum(k2_ref[s], 0)
            direct = lax.dot_general(half_ref[s], y_ref[k2], dims, preferred_element_type=F32)
            weighted = p_ref[k].astype(F32) * v_ref[...]
            high = weighted.astype(BF16)
            low = (weighted - high.astype(F32)).astype(BF16)
            other = p_ref[k2]
            term = lax.dot_general(high, other, dims, preferred_element_type=F32)
            term += lax.dot_general(low, other, dims, preferred_element_type=F32)
            both.append(2.0 * term - direct)
        v = jnp.concatenate(both, axis=1)
        for i in range(n_ga):
            o_ref[i, a] = v[i * quarter : (i + 1) * quarter]
        return carry

    lax.fori_loop(0, n, source, 0)


def tail_kernel(n, rows, per_dev, k2_ref, at_ref, part, out, own, recv1, tsend, recv2, second,
                outbox, inbox, lines, s1, r1, s2, r2, as_, ar, gs, gr):
    greet(n, False, True, True)
    begin, middle, end = reduce_two(part, own, recv1, tsend, recv2, s1, r1, s2, r2, 1)
    begin()
    me = lax.axis_index("ka")
    g = lax.axis_index("ga")
    n_ga = out.shape[0]
    shape = own.shape[1:]
    nt = shape[1] // CAPQ
    left = lax.broadcasted_iota(jnp.int32, shape, 1) < nt
    for a in range(n):
        second[a] = jnp.where(left, k2_ref[a * CAPQ], k2_ref[a * CAPQ + 1])
    middle()
    end()
    pairs = per_dev // 2

    def summed(k):
        total = jnp.zeros(shape, F32)
        for a in range(n):
            total += jnp.where(second[a] == k, own[a], 0.0)
        return total[:, :nt] + total[:, nt:]

    def fill(b, carry):
        outbox[b, 0] = own[b]
        for i in range(pairs):
            k = b * per_dev + i
            outbox[b, 1 + i] = jnp.concatenate([summed(k), summed(k + pairs)], axis=1)
        return carry

    lax.fori_loop(0, n, fill, 0)

    def cross(i):
        to = lax.rem(me + i, n)
        return pltpu.make_async_remote_copy(
            src_ref=outbox.at[to],
            dst_ref=inbox.at[me],
            send_sem=as_.at[i],
            recv_sem=ar.at[i],
            device_id={"ka": to},
            device_id_type=pl.DeviceIdType.MESH,
        )

    for i in range(1, n):
        cross(i).start()
    inbox[me] = outbox[me]
    for i in range(1, n):
        cross(i).wait()

    def tile(j):
        at = at_ref[me * rows + j]
        both = inbox[at // CAPQ, 0]
        return jnp.where(at % CAPQ == 0, both[:, :nt], both[:, nt:])

    for j in range(rows // 2):
        lines[j] = jnp.concatenate([tile(j), tile(j + rows // 2)], axis=1)
    for i in range(pairs):
        total = inbox[0, 1 + i]
        for o in range(1, n):
            total += inbox[o, 1 + i]
        lines[rows // 2 + i] = total
    copies = [
        pltpu.make_async_remote_copy(
            src_ref=lines,
            dst_ref=out.at[g],
            send_sem=gs.at[i],
            recv_sem=gr.at[i],
            device_id={"ga": lax.rem(g + i, n_ga)},
            device_id_type=pl.DeviceIdType.MESH,
        )
        for i in range(1, n_ga)
    ]
    for c in copies:
        c.start()
    out[g] = lines[...]
    for c in copies:
        c.wait()


def per_device(x_dens, y_dens, p_dens, coulomb, screened, pairs, q_slot):
    n = lax.axis_size("ka")
    n_ga = lax.axis_size("ga")
    per_dev, nt, g = x_dens.shape
    q_slots = screened.shape[0]
    rows = pairs.shape[0]
    slots = n * CAPQ
    shape = jax.ShapeDtypeStruct
    listed = jnp.pad(pairs, ((0, 0), (0, 128 - pairs.shape[1]))).reshape(2, rows // 2, 128)
    x_all, listed = pl.pallas_call(
        functools.partial(first_kernel, n),
        out_shape=[shape((n * per_dev, nt, g), BF16), shape((n * 2, rows // 2, 128), jnp.int32)],
        in_specs=[VM, VM],
        out_specs=[VM, VM],
        scratch_shapes=gather_sems(n) + gather_sems(n),
        compiler_params=params(0),
        name="gather_x",
    )(x_dens, listed)
    listed = listed.reshape(n * rows, 128)[:, :3].reshape(n * rows * 3)
    wide = F32 if slots * nt <= 2048 else BF16
    ints = lambda m: shape((m,), jnp.int32)
    part, k_at, k2_at, at = pl.pallas_call(
        functools.partial(half_kernel, n, rows, q_slots),
        out_shape=[shape((n_ga, slots, nt, g), wide), ints(slots), ints(slots), ints(n * rows)],
        in_specs=[SM, SM, VM, VM],
        out_specs=[VM, SM, SM, SM],
        scratch_shapes=[pltpu.SMEM((slots,), jnp.int32), pltpu.SMEM((n,), jnp.int32)],
        compiler_params=pltpu.CompilerParams(vmem_limit_bytes=LIMIT),
        name="half",
    )(listed, q_slot, x_all, screened)
    pieces = 4
    half, y_all, p_all = pl.pallas_call(
        functools.partial(second_kernel, n, pieces),
        out_shape=[shape((slots, nt, g), BF16)] + [shape((n * per_dev, nt, g), BF16)] * 2,
        in_specs=[VM, VM, VM],
        out_specs=[VM, VM, VM],
        scratch_shapes=[
            pltpu.VMEM((2, slots, nt, g), wide),
            pltpu.VMEM((slots, nt, g), BF16),
            pltpu.VMEM((slots, nt, g), BF16),
            pltpu.SemaphoreType.DMA((2 * pieces,)),
            pltpu.SemaphoreType.DMA((2 * pieces,)),
            pltpu.SemaphoreType.DMA((pieces,)),
            pltpu.SemaphoreType.DMA((pieces,)),
        ]
        + gather_sems(n)
        + gather_sems(n),
        compiler_params=params(1),
        name="reduce_gather",
    )(part, y_dens, p_dens)
    quarter = nt // n_ga
    block = pl.pallas_call(
        functools.partial(block_kernel, n),
        out_shape=shape((n_ga, n, quarter, CAPQ * nt), F32),
        in_specs=[SM, SM, VM, VM, VM, VM],
        out_specs=VM,
        compiler_params=pltpu.CompilerParams(vmem_limit_bytes=LIMIT),
        name="block",
    )(k_at, k2_at, half, y_all, p_all, coulomb.reshape(1, g))
    line = (n, quarter, CAPQ * nt)
    lines = rows // 2 + per_dev // 2
    each = line[1:]
    full = pl.pallas_call(
        functools.partial(tail_kernel, n, rows, per_dev),
        out_shape=shape((n_ga, lines) + each, F32),
        in_specs=[SM, SM, VM],
        out_specs=VM,
        scratch_shapes=[
            pltpu.VMEM(line, F32),
            pltpu.VMEM((2,) + line, F32),
            pltpu.VMEM(line, F32),
            pltpu.VMEM(line, F32),
            pltpu.VMEM(line, jnp.int32),
            pltpu.VMEM((n, 1 + per_dev // 2) + each, F32),
            pltpu.VMEM((n, 1 + per_dev // 2) + each, F32),
            pltpu.VMEM((lines,) + each, F32),
        ]
        + [pltpu.SemaphoreType.DMA((2,))] * 4
        + [pltpu.SemaphoreType.DMA((n,))] * 2
        + [pltpu.SemaphoreType.DMA((n_ga,))] * 2,
        compiler_params=params(2),
        name="tail",
    )(k2_at, at, block)
    split = lambda v: jnp.concatenate([v[..., :nt], v[..., nt:]], axis=1)
    blocks = split(full[:, : rows // 2]).transpose(1, 0, 2, 3).reshape(rows, nt * nt)
    mirrored = split(full[:, rows // 2 :]).transpose(1, 3, 0, 2).reshape(per_dev, nt * nt)
    return (blocks, mirrored)


def solution(mesh):
    in_specs = (
        P("ka", None, "ga"),
        P("ka", None, "ga"),
        P("ka", None, "ga"),
        P("ga"),
        P("ka", "ga", None),
        P("ka", None),
        P(),
    )
    out_specs = (P("ka", None), P("ka", None))
    return jax.shard_map(
        per_device, mesh=mesh, in_specs=in_specs, out_specs=out_specs, check_vma=False
    )
```

```python
import functools
import jax
import jax.numpy as jnp
from jax import lax
from jax.experimental import pallas as pl
from jax.experimental.pallas import tpu as pltpu
from jax.sharding import PartitionSpec as P

CAPQ = 2
F32 = jnp.float32
BF16 = jnp.bfloat16
VM = pl.BlockSpec(memory_space=pltpu.VMEM)
SM = pl.BlockSpec(memory_space=pltpu.SMEM)
LIMIT = 66000000


class Gather:
    def __init__(self, n, src, out, send, recv):
        self.n, self.nz = n, n // 2
        self.me = lax.axis_index("ka")
        self.z, self.y = self.me // 2, self.me % 2
        self.src, self.out, self.send, self.recv = src, out, send, recv
        self.size = src.shape[0]
        self.cut = self.size - max(1, self.size // 6)

    def copy(self, zz, yy, half, way, own=False):
        first, length = (self.cut, self.size - self.cut) if half else (0, self.cut)
        block = self.out.at[pl.ds((zz * 2 + yy) * self.size + first, length)]
        source = self.src.at[pl.ds(first, length)] if own else block
        index = (zz * 2 + yy) * 2 + half
        if way == 2:
            target = self.z * 2 + 1 - self.y
        else:
            step = 1 if way == 0 else -1
            target = (self.z + step) * 2 + self.y
        return pltpu.make_async_remote_copy(
            src_ref=source,
            dst_ref=block,
            send_sem=self.send.at[way * 2 * self.n + index],
            recv_sem=self.recv.at[index],
            device_id={"ka": target},
            device_id_type=pl.DeviceIdType.MESH,
        )

    def chain(self, zz, yy, half, act, ways=(0, 1), own=False):
        for way in ways:
            free = self.z < self.nz - 1 if way == 0 else self.z > 0

            @pl.when(free)
            def _(way=way):
                act(self.copy(zz, yy, half, way, own))

    def first(self):
        start = lambda c: c.start()
        self.copy(self.z, self.y, 1, 2, True).start()
        self.chain(self.z, self.y, 0, start, own=True)
        self.chain(self.z, self.y, 1, start, own=True)
        self.copy(self.z, self.y, 0, 2, True).start()
        self.out[pl.ds(self.me * self.size, self.size)] = self.src[...]

    def second(self):
        start = lambda c: c.start()
        self.copy(self.z, 1 - self.y, 1, 2).wait_recv()
        self.chain(self.z, 1 - self.y, 1, start)

    def hop(self, h):
        start = lambda c: c.start()
        for way in (0, 1):
            zz = self.z - h if way == 0 else self.z + h
            there = zz >= 0 if way == 0 else zz < self.nz

            @pl.when(there)
            def _(zz=zz, way=way):
                for yy, half in ((self.y, 0), (self.y, 1), (1 - self.y, 1)):
                    self.copy(zz, yy, half, 2).wait_recv()
                    self.chain(zz, yy, half, start, (way,))
                    if half == 0:
                        self.copy(zz, yy, 0, 2).start()

    def finish(self):
        done = lambda c: c.wait_send()
        self.copy(self.z, self.y, 1, 2, True).wait_send()
        for half in (0, 1):
            self.chain(self.z, self.y, half, done, own=True)
        self.copy(self.z, self.y, 0, 2, True).wait_send()
        self.chain(self.z, 1 - self.y, 1, done)
        self.copy(self.z, 1 - self.y, 0, 2).wait_recv()

        def tail(h, carry):
            for way in (0, 1):
                zz = self.z - h if way == 0 else self.z + h
                there = zz >= 0 if way == 0 else zz < self.nz

                @pl.when(there)
                def _(zz=zz, way=way):
                    for yy, half in ((self.y, 0), (self.y, 1), (1 - self.y, 1)):
                        self.chain(zz, yy, half, done, (way,))
                    self.copy(zz, self.y, 0, 2).wait_send()
                    self.copy(zz, 1 - self.y, 0, 2).wait_recv()

            return carry

        lax.fori_loop(1, self.nz, tail, 0)


def run_gathers(gathers):
    for g in gathers:
        g.first()
    for g in gathers:
        g.second()

    def body(h, carry):
        for g in gathers:
            g.hop(h)
        return carry

    lax.fori_loop(1, gathers[0].nz, body, 0)
    for g in gathers:
        g.finish()


def greet(n, ka_too, ga_too, all_ka=False):
    barrier = pltpu.get_barrier_semaphore()
    me = lax.axis_index("ka")
    z, y = me // 2, me % 2
    nz = n // 2
    targets = []
    if ka_too:
        targets += [{"ka": lax.rem(z + 1, nz) * 2 + y}, {"ka": lax.rem(z + nz - 1, nz) * 2 + y}]
        targets += [{"ka": z * 2 + 1 - y}]
    if all_ka:
        targets += [{"ka": lax.rem(me + i, n)} for i in range(1, n)]
    if ga_too:
        g = lax.axis_index("ga")
        n_ga = lax.axis_size("ga")
        targets += [{"ga": lax.rem(g + i, n_ga)} for i in range(1, n_ga)]
    for t in targets:
        pl.semaphore_signal(barrier, inc=1, device_id=t, device_id_type=pl.DeviceIdType.MESH)
    pl.semaphore_wait(barrier, len(targets))


def gather_sems(n):
    return [pltpu.SemaphoreType.DMA((6 * n,)), pltpu.SemaphoreType.DMA((2 * n,))]


def params(collective_id):
    return pltpu.CompilerParams(
        collective_id=collective_id, has_side_effects=True, vmem_limit_bytes=LIMIT
    )


def first_kernel(n, x_ref, l_ref, xo_ref, lo_ref, xs, xr, ls, lr):
    greet(n, True, False)
    run_gathers([Gather(n, l_ref, lo_ref, ls, lr), Gather(n, x_ref, xo_ref, xs, xr)])


def table_kernel(n, rows, q_slots, list_ref, qs_ref, k_ref, k2_ref, at_ref, w_at, count):
    me = lax.axis_index("ka")
    slots = n * CAPQ

    def clear(s, c):
        k_ref[s] = 0
        k2_ref[s] = -1
        w_at[s] = 0
        return c

    lax.fori_loop(0, slots, clear, 0)

    def source(a, c):
        def zero(o, c):
            count[o] = 0
            return c

        lax.fori_loop(0, n, zero, 0)

        def pair(j, c):
            r = a * rows + j
            slot = qs_ref[list_ref[r * 3 + 2]]
            owner = slot // q_slots
            rank = count[owner]
            count[owner] = rank + 1
            at_ref[r] = owner * CAPQ + rank

            @pl.when(owner == me)
            def _():
                s = a * CAPQ + rank
                k_ref[s] = list_ref[r * 3]
                k2_ref[s] = list_ref[r * 3 + 1]
                w_at[s] = slot % q_slots

            return c

        return lax.fori_loop(0, rows, pair, c)

    lax.fori_loop(0, n, source, 0)


def reduce_two(part, out, recv1, tsend, recv2, s1, r1, s2, r2, pieces):
    g = lax.axis_index("ga")
    x, c = g // 2, g % 2
    per = part.shape[1] // pieces
    there, here = 1 - x, x

    def one(t, xx, i):
        rows = pl.ds(i * per, per)
        return pltpu.make_async_remote_copy(
            src_ref=part.at[xx * 2 + 1 - c, rows],
            dst_ref=recv1.at[xx, rows],
            send_sem=s1.at[t * pieces + i],
            recv_sem=r1.at[t * pieces + i],
            device_id={"ga": x * 2 + 1 - c},
            device_id_type=pl.DeviceIdType.MESH,
        )

    def two(i):
        rows = pl.ds(i * per, per)
        return pltpu.make_async_remote_copy(
            src_ref=tsend.at[rows],
            dst_ref=recv2.at[rows],
            send_sem=s2.at[i],
            recv_sem=r2.at[i],
            device_id={"ga": there * 2 + c},
            device_id_type=pl.DeviceIdType.MESH,
        )

    def begin(i):
        one(0, there, i).start()
        one(1, here, i).start()

    def middle():
        for i in range(pieces):
            rows = pl.ds(i * per, per)
            one(0, there, i).wait_recv()
            v = part[there * 2 + c, rows].astype(F32) + recv1[there, rows].astype(F32)
            tsend[rows] = v.astype(tsend.dtype)
            two(i).start()

    def end():
        for i in range(pieces):
            rows = pl.ds(i * per, per)
            one(1, here, i).wait_recv()
            two(i).wait_recv()
            v = part[here * 2 + c, rows].astype(F32) + recv1[here, rows].astype(F32)
            out[rows] = (v + recv2[rows].astype(F32)).astype(out.dtype)
        for i in range(pieces):
            one(0, there, i).wait_send()
            one(1, here, i).wait_send()
            two(i).wait_send()

    return begin, middle, end


def second_kernel(n, pieces, k_ref, w_at, x_ref, w_ref, y_ref, p_ref, half_ref, yo_ref, po_ref, part,
                  recv1, tsend, recv2, s1, r1, s2, r2, ys, yr, ps, pr):
    greet(n, True, True)
    gathers = [Gather(n, y_ref, yo_ref, ys, yr), Gather(n, p_ref, po_ref, ps, pr)]
    for g in gathers:
        g.first()
    begin, middle, end = reduce_two(part, half_ref, recv1, tsend, recv2, s1, r1, s2, r2, pieces)
    n_ga, width = part.shape[0], part.shape[3]
    per = part.shape[1] // pieces

    def multiply(s, c):
        v = jnp.dot(x_ref[k_ref[s]], w_ref[w_at[s]], preferred_element_type=F32)
        for i in range(n_ga):
            part[i, s] = v[:, i * width : (i + 1) * width].astype(part.dtype)
        return c

    for i in range(pieces):
        if i == pieces // 2:
            for g in gathers:
                g.second()
        lax.fori_loop(i * per, (i + 1) * per, multiply, 0)
        begin(i)
    middle()

    def body(h, carry):
        for g in gathers:
            g.hop(h)
        return carry

    lax.fori_loop(1, gathers[0].nz, body, 0)
    for g in gathers:
        g.finish()
    end()


def block_kernel(n, k_ref, k2_ref, half_ref, y_ref, p_ref, v_ref, o_ref):
    n_ga, quarter = o_ref.shape[0], o_ref.shape[2]
    dims = (((1,), (1,)), ((), ()))

    def source(a, carry):
        both = []
        for c in range(CAPQ):
            s = a * CAPQ + c
            k, k2 = k_ref[s], jnp.maximum(k2_ref[s], 0)
            direct = lax.dot_general(half_ref[s], y_ref[k2], dims, preferred_element_type=F32)
            weighted = p_ref[k].astype(F32) * v_ref[...]
            high = weighted.astype(BF16)
            low = (weighted - high.astype(F32)).astype(BF16)
            other = p_ref[k2]
            term = lax.dot_general(high, other, dims, preferred_element_type=F32)
            term += lax.dot_general(low, other, dims, preferred_element_type=F32)
            both.append(2.0 * term - direct)
        v = jnp.concatenate(both, axis=1)
        for i in range(n_ga):
            o_ref[i, a] = v[i * quarter : (i + 1) * quarter]
        return carry

    lax.fori_loop(0, n, source, 0)


def tail_kernel(n, rows, per_dev, k2_ref, at_ref, part, out, own, recv1, tsend, recv2, second,
                outbox, inbox, lines, s1, r1, s2, r2, as_, ar, gs, gr):
    greet(n, False, True, True)
    begin, middle, end = reduce_two(part, own, recv1, tsend, recv2, s1, r1, s2, r2, 1)
    begin(0)
    me = lax.axis_index("ka")
    g = lax.axis_index("ga")
    n_ga = out.shape[0]
    shape = own.shape[1:]
    nt = shape[1] // CAPQ
    left = lax.broadcasted_iota(jnp.int32, shape, 1) < nt
    for a in range(n):
        second[a] = jnp.where(left, k2_ref[a * CAPQ], k2_ref[a * CAPQ + 1])
    middle()
    end()
    pairs = per_dev // 2

    def summed(k):
        total = jnp.zeros(shape, F32)
        for a in range(n):
            total += jnp.where(second[a] == k, own[a], 0.0)
        return total[:, :nt] + total[:, nt:]

    def fill(b, carry):
        outbox[b, 0] = own[b]
        for i in range(pairs):
            k = b * per_dev + i
            outbox[b, 1 + i] = jnp.concatenate([summed(k), summed(k + pairs)], axis=1)
        return carry

    lax.fori_loop(0, n, fill, 0)

    def cross(i):
        to = lax.rem(me + i, n)
        return pltpu.make_async_remote_copy(
            src_ref=outbox.at[to],
            dst_ref=inbox.at[me],
            send_sem=as_.at[i],
            recv_sem=ar.at[i],
            device_id={"ka": to},
            device_id_type=pl.DeviceIdType.MESH,
        )

    for i in range(1, n):
        cross(i).start()
    inbox[me] = outbox[me]
    for i in range(1, n):
        cross(i).wait()

    def tile(j):
        at = at_ref[me * rows + j]
        both = inbox[at // CAPQ, 0]
        return jnp.where(at % CAPQ == 0, both[:, :nt], both[:, nt:])

    for j in range(rows // 2):
        lines[j] = jnp.concatenate([tile(j), tile(j + rows // 2)], axis=1)
    for i in range(pairs):
        total = inbox[0, 1 + i]
        for o in range(1, n):
            total += inbox[o, 1 + i]
        lines[rows // 2 + i] = total
    copies = [
        pltpu.make_async_remote_copy(
            src_ref=lines,
            dst_ref=out.at[g],
            send_sem=gs.at[i],
            recv_sem=gr.at[i],
            device_id={"ga": lax.rem(g + i, n_ga)},
            device_id_type=pl.DeviceIdType.MESH,
        )
        for i in range(1, n_ga)
    ]
    for c in copies:
        c.start()
    out[g] = lines[...]
    for c in copies:
        c.wait()


def per_device(x_dens, y_dens, p_dens, coulomb, screened, pairs, q_slot):
    n = lax.axis_size("ka")
    n_ga = lax.axis_size("ga")
    per_dev, nt, g = x_dens.shape
    q_slots = screened.shape[0]
    rows = pairs.shape[0]
    slots = n * CAPQ
    shape = jax.ShapeDtypeStruct
    listed = jnp.pad(pairs, ((0, 0), (0, 128 - pairs.shape[1]))).reshape(2, rows // 2, 128)
    x_all, listed = pl.pallas_call(
        functools.partial(first_kernel, n),
        out_shape=[shape((n * per_dev, nt, g), BF16), shape((n * 2, rows // 2, 128), jnp.int32)],
        in_specs=[VM, VM],
        out_specs=[VM, VM],
        scratch_shapes=gather_sems(n) + gather_sems(n),
        compiler_params=params(0),
        name="gather_x",
    )(x_dens, listed)
    listed = listed.reshape(n * rows, 128)[:, :3].reshape(n * rows * 3)
    wide = F32 if slots * nt <= 2048 else BF16
    ints = lambda m: shape((m,), jnp.int32)
    k_at, k2_at, at, w_at = pl.pallas_call(
        functools.partial(table_kernel, n, rows, q_slots),
        out_shape=[ints(slots), ints(slots), ints(n * rows), ints(slots)],
        in_specs=[SM, SM],
        out_specs=[SM] * 4,
        scratch_shapes=[pltpu.SMEM((n,), jnp.int32)],
        name="tables",
    )(listed, q_slot)
    pieces = 4
    half, y_all, p_all = pl.pallas_call(
        functools.partial(second_kernel, n, pieces),
        out_shape=[shape((slots, nt, g), BF16)] + [shape((n * per_dev, nt, g), BF16)] * 2,
        in_specs=[SM, SM, VM, VM, VM, VM],
        out_specs=[VM, VM, VM],
        scratch_shapes=[
            pltpu.VMEM((n_ga, slots, nt, g), wide),
            pltpu.VMEM((2, slots, nt, g), wide),
            pltpu.VMEM((slots, nt, g), BF16),
            pltpu.VMEM((slots, nt, g), BF16),
            pltpu.SemaphoreType.DMA((2 * pieces,)),
            pltpu.SemaphoreType.DMA((2 * pieces,)),
            pltpu.SemaphoreType.DMA((pieces,)),
            pltpu.SemaphoreType.DMA((pieces,)),
        ]
        + gather_sems(n)
        + gather_sems(n),
        compiler_params=params(1),
        name="reduce_gather",
    )(k_at, w_at, x_all, screened, y_dens, p_dens)
    quarter = nt // n_ga
    block = pl.pallas_call(
        functools.partial(block_kernel, n),
        out_shape=shape((n_ga, n, quarter, CAPQ * nt), F32),
        in_specs=[SM, SM, VM, VM, VM, VM],
        out_specs=VM,
        compiler_params=pltpu.CompilerParams(vmem_limit_bytes=LIMIT),
        name="block",
    )(k_at, k2_at, half, y_all, p_all, coulomb.reshape(1, g))
    line = (n, quarter, CAPQ * nt)
    lines = rows // 2 + per_dev // 2
    each = line[1:]
    full = pl.pallas_call(
        functools.partial(tail_kernel, n, rows, per_dev),
        out_shape=shape((n_ga, lines) + each, F32),
        in_specs=[SM, SM, VM],
        out_specs=VM,
        scratch_shapes=[
            pltpu.VMEM(line, F32),
            pltpu.VMEM((2,) + line, F32),
            pltpu.VMEM(line, F32),
            pltpu.VMEM(line, F32),
            pltpu.VMEM(line, jnp.int32),
            pltpu.VMEM((n, 1 + per_dev // 2) + each, F32),
            pltpu.VMEM((n, 1 + per_dev // 2) + each, F32),
            pltpu.VMEM((lines,) + each, F32),
        ]
        + [pltpu.SemaphoreType.DMA((2,))] * 4
        + [pltpu.SemaphoreType.DMA((n,))] * 2
        + [pltpu.SemaphoreType.DMA((n_ga,))] * 2,
        compiler_params=params(2),
        name="tail",
    )(k2_at, at, block)
    split = lambda v: jnp.concatenate([v[..., :nt], v[..., nt:]], axis=1)
    blocks = split(full[:, : rows // 2]).transpose(1, 0, 2, 3).reshape(rows, nt * nt)
    mirrored = split(full[:, rows // 2 :]).transpose(1, 3, 0, 2).reshape(per_dev, nt * nt)
    return (blocks, mirrored)


def solution(mesh):
    in_specs = (
        P("ka", None, "ga"),
        P("ka", None, "ga"),
        P("ka", None, "ga"),
        P("ga"),
        P("ka", "ga", None),
        P("ka", None),
        P(),
    )
    out_specs = (P("ka", None), P("ka", None))
    return jax.shard_map(
        per_device, mesh=mesh, in_specs=in_specs, out_specs=out_specs, check_vma=False
    )
```
